32 devices in a mesh: rows: 8 (over y, x, core), hub: 4 (over z).
Axes of the slice: x: 2, y: 2, z: 4, core: 2. Of those that a mesh axis runs over, the one named last changes fastest.
Arguments:
- tail_blocks: float32 [2304, 128, 128], P(('rows', 'hub')), may hold values from -0.21875 to 0.21875
- tail_row: int32 [2304], P(('rows', 'hub')), may hold values from 0 to 15
- tail_owner: int32 [2304, 1], P(('rows', 'hub')), may hold values from 0 to 7; in each aligned block of 72 rows (0 to 71, 72 to 143, ...) at most 27 rows name the same one
- tail_slot: int32 [2304], P(('rows', 'hub')), may hold values from 0 to 63
- hub_blocks: float32 [768, 128, 128], P(('rows', 'hub')), may hold values from -0.21875 to 0.21875
- hub_row: int32 [768], P(('rows', 'hub')), may hold values from 0 to 15
- hub_col: int32 [768], P(('rows', 'hub')), may hold values from 0 to 127
- x_tail: float32 [2048, 128], P(('rows', 'hub')), may hold values from 0 to 0.5
- cost_tail: float32 [2048, 128], P(('rows', 'hub')), may hold values from -6 to 6
- upper_tail: float32 [2048, 128], P(('rows', 'hub')), may hold values from 0.5 to 2
- x_hub: float32 [128, 128], P('hub'), may hold values from 0 to 0.5
- cost_hub: float32 [128, 128], P('hub'), may hold values from -6 to 6
- upper_hub: float32 [128, 128], P('hub'), may hold values from 0.5 to 2
- duals: float32 [512, 128], P(('rows', 'hub')), may hold values from 0 to 1
- demand: float32 [512, 128], P(('rows', 'hub')), may hold values from -6 to 6
Outputs:
- x_tail_out: float32 [2048, 128], P(('rows', 'hub'))
- x_hub_out: float32 [128, 128], P('hub')
- duals_out: float32 [512, 128], P(('rows', 'hub'))
The draws below stay inside these ranges and needn't reach their ends.
Inputs may be any that keep to these rules, and one draw needn't show every extreme that they name: `tail_owner`: among the blocks of one device no owner is named more than 27 times; on some device one owner is named exactly 27 times.
All inputs are finite; a program needn't handle non-finite values.
Results may differ from the reference program's by a relative error of at most 0.0001.
Values sent between devices are 32-bit elements; how exact they have to be, the bound alone decides.
No kernel may reach another device: no remote copies, remote signals or barrier semaphores. Data moves between devices by JAX's collectives and lax.ppermute only.
A program may use at most 64 MiB of HBM per device.

```python
import math
import jax
import jax.numpy as jnp
import numpy as np
from jax import lax

BW = 128
NB_DEV = 72
HNB_DEV = 24
CB_DEV = 64
RB_DEV = 16
ITERS = 3
CAP = 27
TAILB = 2048
HUBB = 128
ROWB = 512
TAILN = 2304
HUBN = 768
N_ROWS = 8
N_HUB = 4


def place_ends(entries, rng, low, largest):
    extent = entries.shape
    index_at = [jax.random.randint(jax.random.fold_in(rng, axis), (), 0, extent[axis]) for axis in range(len(extent))]
    entries = entries.at[tuple(index_at)].set(low)
    longest = extent.index(max(extent))
    index_at[longest] = (index_at[longest] + 1) % extent[longest]
    return entries.at[tuple(index_at)].set(largest)


def block_levels(stream_key, dims, split, smallest, high):
    gain, own = 1.0, jax.random.fold_in(stream_key, 6)
    for axis_at, blocks in split:
        heights = jnp.exp(jax.random.uniform(jax.random.fold_in(own, axis_at), (blocks,), jnp.float32, smallest / len(split), high / len(split)))
        gain = gain * jnp.repeat(heights, dims[axis_at] // blocks).reshape([-1 if axis == axis_at else 1 for axis in range(len(dims))])
    return gain


def rank_bounds(number_of, skew):
    portions = [(1 << 20) // math.isqrt(standing ** skew) + 1 for standing in range(1, number_of + 1)]
    deviation = 1 + sum(portions) // (1 << 30)
    return np.cumsum(np.array([max(1, weight // deviation) for weight in portions]))


def skewed_ids(rng, extent, count, lean):
    table = rank_bounds(count, lean)
    ticket = jax.random.randint(jax.random.fold_in(rng, 1), extent, 0, int(table[count - 1]))
    rank = jnp.searchsorted(jnp.asarray(table, jnp.int32), ticket, side="right")
    return jax.random.permutation(jax.random.fold_in(rng, 2), count)[rank].astype(jnp.int32)


def deal_out(own_key, own, number, rows, amount, top, most, lean):
    order = jax.random.permutation(own_key, amount)
    heavy_load, ordinary = portions_of(amount, rows * top, most, lean, True), portions_of(amount, rows * top, most, lean, False)
    places = jnp.arange(amount)

    def named(sizes, turn):
        used = int((sizes > 0).sum())
        fixed = max(1, used // 4)
        shifted = fixed + (places - fixed + turn * (used - fixed)) % max(1, amount - fixed)
        return jnp.zeros((amount,), jnp.int32).at[order[jnp.where(places < fixed, places, shifted)]].set(jnp.asarray(sizes, jnp.int32))

    sizes = jnp.where(number % 4 == 0, named(heavy_load, number // 4), named(ordinary, number - number // 4 - 1))
    mixed = jax.random.permutation(jax.random.fold_in(own, 3), amount)
    giver, sink = mixed[0:amount // 2 * 2:2], mixed[1:amount // 2 * 2:2]
    margin = jnp.minimum(sizes[giver] - 1, most - sizes[sink]) // 2
    margin = jnp.where((giver == order[0]) | (sink == order[0]) | (sizes[sink] == 0), 0, jnp.maximum(margin, 0))
    shifted = jax.random.randint(jax.random.fold_in(own, 4), (amount // 2,), 0, 1 << 20) % (margin + 1)
    sizes = sizes.at[giver].add(-shifted).at[sink].add(shifted)
    items = jnp.searchsorted(jnp.cumsum(sizes), jnp.arange(rows * top), side="right").astype(jnp.int32)
    table = items.reshape(top, rows).T
    table = table[jax.random.permutation(jax.random.fold_in(own, 1), rows)]
    turn = jax.random.randint(jax.random.fold_in(own, 2), (rows, 1), 0, top)
    return jnp.take_along_axis(table, (jnp.arange(top)[None, :] + turn) % top, axis=1)


def portions_of(amount, total, bound, slope, full):
    weights = [(1 << 20) // math.isqrt(standing ** slope) + 1 for standing in range(1, amount + 1)]
    largest = bound if full else min(bound, max(-(-total // amount), total * weights[0] // sum(weights)))
    least = 1 if total - largest >= amount - 1 else 0
    given, rest = [largest] + [least] * (amount - 1), total - largest - least * (amount - 1)
    while rest > 0:
        free = [i for i in range(1, amount) if given[i] < largest] or [i for i in range(1, amount) if given[i] < bound]
        mass, budget = sum([weights[i] for i in free]), rest
        for i in free:
            extra = min(bound - given[i], max(1, budget * weights[i] // mass), rest)
            given[i] = given[i] + extra
            rest = rest - extra
    return np.array(given)


def scatter_about(stream_key, shape, spread, bound, split=(), kind=jnp.bfloat16):
    array = spread * jax.random.normal(stream_key, shape, jnp.float32)
    if split:
        array = array * block_levels(stream_key, shape, split, -0.22, 0.18)
    return jnp.clip(array, -bound, bound).astype(kind)


def setup_inputs(seed: int = 0) -> dict:
    arg_keys = jax.random.split(jax.random.key(seed), 16)
    tail_blocks = scatter_about(arg_keys[0], (TAILN, BW, BW), (BW * (NB_DEV + HNB_DEV) // RB_DEV) ** -0.5, 0.21875, ((0, 32),), jnp.float32)
    tail_row = place_ends(jax.random.randint(arg_keys[1], (TAILN,), 0, RB_DEV), jax.random.fold_in(arg_keys[1], 1), 0, RB_DEV - 1).astype(jnp.int32)
    tail_owner_keys = jax.random.split(jax.random.fold_in(arg_keys[2], 1), TAILN // NB_DEV)
    tail_owner_turns = jax.random.permutation(jax.random.fold_in(arg_keys[2], 3), TAILN // NB_DEV)
    tail_owner = jax.vmap(lambda own, number: deal_out(jax.random.fold_in(arg_keys[2], 2), own, number, NB_DEV, N_ROWS, 1, CAP, 2))(tail_owner_keys, tail_owner_turns).reshape((TAILN, 1))
    tail_slot = place_ends(jax.random.randint(arg_keys[3], (TAILN,), 0, CB_DEV), jax.random.fold_in(arg_keys[3], 1), 0, CB_DEV - 1).astype(jnp.int32)
    hub_blocks = scatter_about(arg_keys[4], (HUBN, BW, BW), (BW * (NB_DEV + HNB_DEV) // RB_DEV) ** -0.5, 0.21875, ((0, 32),), jnp.float32)
    hub_row = place_ends(jax.random.randint(arg_keys[5], (HUBN,), 0, RB_DEV), jax.random.fold_in(arg_keys[5], 1), 0, RB_DEV - 1).astype(jnp.int32)
    hub_col = place_ends(skewed_ids(arg_keys[6], (HUBN,), HUBB, 2), jax.random.fold_in(arg_keys[6], 3), 0, HUBB - 1).astype(jnp.int32)
    x_tail = jnp.clip(0.5 * jax.random.uniform(arg_keys[7], (TAILB, BW), jnp.float32) ** block_levels(arg_keys[7], (TAILB, BW), ((0, 32),), -0.2, 0.2), 0.0, 0.5)
    cost_tail = scatter_about(arg_keys[8], (TAILB, BW), 1.0, 6.0, ((0, 32),), jnp.float32)
    upper_tail = jnp.clip(jnp.exp(math.log(2.0) - 1.3862944 * jax.random.uniform(arg_keys[9], (TAILB, BW), jnp.float32) ** block_levels(arg_keys[9], (TAILB, BW), ((0, 32),), -0.2, 0.2)), 0.5, 2.0)
    x_hub = jnp.clip(0.5 * jax.random.uniform(arg_keys[10], (HUBB, BW), jnp.float32) ** block_levels(arg_keys[10], (HUBB, BW), ((0, 4),), -0.2, 0.2), 0.0, 0.5)
    cost_hub = scatter_about(arg_keys[11], (HUBB, BW), 1.0, 6.0, ((0, 4),), jnp.float32)
    upper_hub = jnp.clip(jnp.exp(math.log(2.0) - 1.3862944 * jax.random.uniform(arg_keys[12], (HUBB, BW), jnp.float32) ** block_levels(arg_keys[12], (HUBB, BW), ((0, 4),), -0.2, 0.2)), 0.5, 2.0)
    duals = jnp.clip(1.0 * jax.random.uniform(arg_keys[13], (ROWB, BW), jnp.float32) ** block_levels(arg_keys[13], (ROWB, BW), ((0, 32),), -0.2, 0.2), 0.0, 1.0)
    demand = scatter_about(arg_keys[14], (ROWB, BW), 1.0, 6.0, ((0, 32),), jnp.float32)
    return dict(tail_blocks=tail_blocks, tail_row=tail_row, tail_owner=tail_owner, tail_slot=tail_slot, hub_blocks=hub_blocks, hub_row=hub_row, hub_col=hub_col, x_tail=x_tail, cost_tail=cost_tail, upper_tail=upper_tail, x_hub=x_hub, cost_hub=cost_hub, upper_hub=upper_hub, duals=duals, demand=demand)


primal_step = 0.25
dual_step = 0.25


def forward_product(blocks, row_index, col_index, vector, row_count):
    picked = vector[col_index]
    product = jnp.einsum("bij,bj->bi", blocks, picked, precision=lax.Precision.HIGHEST)
    return jax.ops.segment_sum(product, row_index, num_segments=row_count)


def adjoint_product(blocks, row_index, col_index, weights, col_count):
    picked = weights[row_index]
    product = jnp.einsum("bij,bi->bj", blocks, picked, precision=lax.Precision.HIGHEST)
    return jax.ops.segment_sum(product, col_index, num_segments=col_count)


def reference(tail_blocks, tail_row, tail_owner, tail_slot, hub_blocks, hub_row, hub_col, x_tail, cost_tail, upper_tail, x_hub, cost_hub, upper_hub, duals, demand):
    tail_count = tail_blocks.shape[0]
    hub_count = hub_blocks.shape[0]
    row_count = duals.shape[0]
    device_of = (jnp.arange(tail_count, dtype=jnp.int32) // NB_DEV).astype(jnp.int32)
    tail_rows = (device_of * RB_DEV + tail_row).astype(jnp.int32)
    tail_cols = ((tail_owner[:, 0] * N_HUB + device_of % N_HUB) * CB_DEV + tail_slot).astype(jnp.int32)
    hub_device = (jnp.arange(hub_count, dtype=jnp.int32) // HNB_DEV).astype(jnp.int32)
    hub_rows = (hub_device * RB_DEV + hub_row).astype(jnp.int32)
    hub_cols = hub_col.astype(jnp.int32)
    for iteration in range(ITERS):
        image_tail = adjoint_product(tail_blocks, tail_rows, tail_cols, duals, x_tail.shape[0])
        image_hub = adjoint_product(hub_blocks, hub_rows, hub_cols, duals, x_hub.shape[0])
        tail_next = jnp.minimum(jnp.maximum(x_tail - primal_step * (cost_tail - image_tail), 0.0), upper_tail)
        hub_next = jnp.minimum(jnp.maximum(x_hub - primal_step * (cost_hub - image_hub), 0.0), upper_hub)
        tail_extra = 2.0 * tail_next - x_tail
        hub_extra = 2.0 * hub_next - x_hub
        primal_image = forward_product(tail_blocks, tail_rows, tail_cols, tail_extra, row_count)
        primal_image = primal_image + forward_product(hub_blocks, hub_rows, hub_cols, hub_extra, row_count)
        duals = jnp.maximum(duals + dual_step * (demand - primal_image), 0.0)
        x_tail = tail_next
        x_hub = hub_next
    return (x_tail, x_hub, duals)
```

```python
import functools

import jax
import jax.numpy as jnp
from jax import lax
from jax.experimental import pallas as pl
from jax.experimental.pallas import tpu as pltpu
from jax.sharding import PartitionSpec as P

ITERS = 3

primal_step = 0.25
dual_step = 0.25

VMEM = pltpu.MemorySpace.VMEM
SMEM = pltpu.MemorySpace.SMEM


def eye_mask(width):
    rows = lax.broadcasted_iota(jnp.int32, (width, width), 0)
    return rows == lax.broadcasted_iota(jnp.int32, (width, width), 1)


def fill_wide(diagonal, wide, width):
    eye = eye_mask(width)
    for r in range(wide.shape[0]):
        spread = jnp.where(eye, diagonal[r : r + 1, :], 0.0)
        wide[r] = jnp.broadcast_to(jnp.sum(spread, axis=1, keepdims=True), (width, width))


def adjoint_terms(blocks, block_row, wide, out):
    def step(b, _):
        product = blocks[b] * wide[block_row[b]]
        out[pl.ds(b, 1), :] = jnp.sum(product, axis=0, keepdims=True)
        return 0

    lax.fori_loop(0, blocks.shape[0], step, 0, unroll=4)


def forward_sums(blocks, block_row, extra, first, sums):
    def step(b, _):
        sums[block_row[b]] += blocks[b] * extra[pl.ds(first + b, 1), :]
        return 0

    lax.fori_loop(0, blocks.shape[0], step, 0, unroll=4)


def first_kernel(tail_row, hub_row, tail_blocks, hub_blocks, duals, tail_out, hub_out, wide):
    fill_wide(duals[...], wide, duals.shape[1])
    adjoint_terms(hub_blocks, hub_row, wide, hub_out)
    adjoint_terms(tail_blocks, tail_row, wide, tail_out)


def split3(values):
    high = values.astype(jnp.bfloat16)
    rest = values - high.astype(jnp.float32)
    middle = rest.astype(jnp.bfloat16)
    low = (rest - middle.astype(jnp.float32)).astype(jnp.bfloat16)
    return high, middle, low


def gathered_image(near, far, slots, stride, share, id_rows, keys):
    tiles = len(id_rows[0])
    image = None
    for slot in range(2 * slots):
        source = near if slot < slots else far
        start = (slot % slots) * stride
        values = source[start : start + share, :]
        match = jnp.concatenate([keys == id_rows[slot][t] for t in range(tiles)], axis=1)[:, :share]
        match = jnp.where(match, 1.0, 0.0).astype(jnp.bfloat16)
        for part in split3(values):
            term = jnp.dot(match, part, preferred_element_type=jnp.float32)
            image = term if image is None else image + term
    return image


def step_kernel(first, last, sizes, *refs):
    slots, share, stride, tail_n, tail_own, hub_n, hub_own, tiles = sizes
    refs = list(refs)
    take = lambda n: [refs.pop(0) for _ in range(n)]
    tail_row, hub_row = take(2)
    if first:
        tail_core, tail_place, hub_place = take(3)
    tail_blocks, hub_blocks, near, far, keys, duals, demand = take(7)
    if first:
        near_state, far_state, hub_state = take(3)
    else:
        x_in, cost, upper, ids = take(4)
    if last:
        tail_x, hub_x, duals_out = take(3)
    else:
        tail_out, hub_out, x_out, duals_out = take(4)
        if first:
            cost, upper, ids = take(3)
    sums, wide, extra = take(3)
    width = duals.shape[1]

    if first:
        for slot in range(2 * slots):
            source = near if slot < slots else far
            start = (slot % slots) * stride + share
            ids[slot * tiles : (slot + 1) * tiles, :] = source[start : start + tiles, :]
        x_in = x_out
        own = tail_n + tail_own
        for which, target in enumerate((x_in, cost, upper)):
            target[tail_n:own, :] = near_state[which * tail_own : (which + 1) * tail_own, :]
            target[own + hub_n :, :] = hub_state[which * hub_own : (which + 1) * hub_own, :]

        def pick_tail(b, _):
            for which, target in enumerate((x_in, cost, upper)):
                at = pl.ds(tail_place[b] + which * tail_own, 1)
                target[pl.ds(b, 1), :] = jnp.where(tail_core[b] == 0, near_state[at, :], far_state[at, :])
            return 0

        def pick_hub(b, _):
            for which, target in enumerate((x_in, cost, upper)):
                at = pl.ds(hub_place[b] + which * hub_own, 1)
                target[pl.ds(own + b, 1), :] = hub_state[at, :]
            return 0

        lax.fori_loop(0, tail_n, pick_tail, 0, unroll=4)
        lax.fori_loop(0, hub_n, pick_hub, 0, unroll=4)

    id_rows = [
        [ids[slot * tiles + t : slot * tiles + t + 1, :] for t in range(tiles)] for slot in range(2 * slots)
    ]
    image = gathered_image(near, far, slots, stride, share, id_rows, keys[...])
    x_old = x_in[...]
    x_new = jnp.minimum(jnp.maximum(x_old - primal_step * (cost[...] - image), 0.0), upper[...])
    extra[...] = 2.0 * x_new - x_old
    if last:
        tail_x[...] = x_new[tail_n : tail_n + tail_own, :]
        hub_x[...] = x_new[tail_n + tail_own + hub_n :, :]
    else:
        x_out[...] = x_new

    eye = eye_mask(width)
    base = duals[...] + dual_step * demand[...]
    scale = -1.0 / dual_step
    for r in range(sums.shape[0]):
        sums[r] = jnp.where(eye, scale * base[r : r + 1, :], 0.0)
    forward_sums(hub_blocks, hub_row, extra, tail_n + tail_own, sums)
    forward_sums(tail_blocks, tail_row, extra, 0, sums)
    for r in range(sums.shape[0]):
        total = jnp.sum(sums[r], axis=1, keepdims=True)
        value = jnp.broadcast_to(jnp.maximum(-dual_step * total, 0.0), (width, width))
        wide[r] = value
        duals_out[r : r + 1, :] = jnp.sum(jnp.where(eye, value, 0.0), axis=0, keepdims=True)
    if not last:
        adjoint_terms(hub_blocks, hub_row, wide, hub_out)
        adjoint_terms(tail_blocks, tail_row, wide, tail_out)


def call(kernel, smem, vmem, outs, scratch, flops):
    return pl.pallas_call(
        kernel,
        out_shape=[jax.ShapeDtypeStruct(s, jnp.float32) for s in outs],
        in_specs=[pl.BlockSpec(memory_space=SMEM)] * len(smem) + [pl.BlockSpec(memory_space=VMEM)] * len(vmem),
        out_specs=[pl.BlockSpec(memory_space=VMEM)] * len(outs),
        scratch_shapes=[pltpu.VMEM(s, jnp.float32) for s in scratch],
        compiler_params=pltpu.CompilerParams(vmem_limit_bytes=40 * 1024 * 1024),
        cost_estimate=pl.CostEstimate(flops=flops, bytes_accessed=0, transcendentals=0),
    )(*smem, *vmem)


def on_device(
    tail_blocks,
    tail_row,
    tail_owner,
    tail_slot,
    hub_blocks,
    hub_row,
    hub_col,
    x_tail,
    cost_tail,
    upper_tail,
    x_hub,
    cost_hub,
    upper_hub,
    duals,
    demand,
):
    row_devs = lax.axis_size("rows")
    hub_devs = lax.axis_size("hub")
    my_row = lax.axis_index("rows")
    my_hub = lax.axis_index("hub")
    tail_n, width = tail_blocks.shape[0], tail_blocks.shape[2]
    hub_n = hub_blocks.shape[0]
    tail_own = x_tail.shape[0]
    hub_own = x_hub.shape[0]
    row_n = duals.shape[0]
    chips = row_devs // 2
    assert row_devs & (row_devs - 1) == 0 and hub_devs & (hub_devs - 1) == 0

    def swap(value, axis, mask):
        count = lax.axis_size(axis)
        return lax.ppermute(value, axis, [(i, i ^ mask) for i in range(count)])

    def over_rows(value):
        near = jnp.concatenate([value] + [swap(value, "rows", 2 * m) for m in range(1, chips)], axis=0)
        return near, swap(near, "rows", 1)

    def over_hub(value):
        return [value] + [swap(value, "hub", m) for m in range(1, hub_devs)]

    share = tail_n + hub_devs * hub_n
    tiles = -(-share // width)
    id_pad = -(-tiles // 8) * 8

    hub_ids = (row_devs * tail_own + hub_col).astype(jnp.float32)
    hub_id_row = jnp.pad(hub_ids[None, :], ((0, 7), (0, width - hub_n)), constant_values=-1.0)
    hub_all = over_hub(jnp.concatenate([x_hub, cost_hub, upper_hub, hub_id_row], axis=0))
    near_state, far_state = over_rows(jnp.concatenate([x_tail, cost_tail, upper_tail], axis=0))
    hub_state = jnp.concatenate([part[: 3 * hub_own] for part in hub_all], axis=0)
    owners = tail_owner[:, 0]
    tail_ids = (owners * tail_own + tail_slot).astype(jnp.float32)
    id_block = jnp.concatenate([tail_ids] + [part[3 * hub_own, :hub_n] for part in hub_all])
    id_block = jnp.pad(id_block, (0, id_pad * width - share), constant_values=-1.0).reshape(id_pad, width)

    relative = owners ^ my_row
    tail_core = relative & 1
    tail_place = (relative >> 1) * (3 * tail_own) + tail_slot
    hub_place = ((hub_col // hub_own) ^ my_hub) * (3 * hub_own) + hub_col % hub_own
    keys = jnp.concatenate(
        [
            tail_ids,
            (my_row * tail_own + jnp.arange(tail_own)).astype(jnp.float32),
            hub_ids,
            (row_devs * tail_own + my_hub * hub_own + jnp.arange(hub_own)).astype(jnp.float32),
        ]
    )
    key_n = keys.shape[0]
    keys = jnp.broadcast_to(keys[:, None], (key_n, width))

    block_work = 2 * (tail_n + hub_n) * width * width
    big = (row_n, width, width)
    tail_terms, hub_terms = call(
        first_kernel,
        (tail_row, hub_row),
        (tail_blocks, hub_blocks, duals),
        [(tail_n, width), (hub_n, width)],
        [big],
        block_work,
    )
    for iteration in range(ITERS):
        first, last = iteration == 0, iteration == ITERS - 1
        parts = [tail_terms] + over_hub(hub_terms)
        near, far = over_rows(jnp.concatenate(parts + [id_block] * first, axis=0))
        stride = share + id_pad * first
        sizes = (chips, share, stride, tail_n, tail_own, hub_n, hub_own, tiles)
        smem = (tail_row, hub_row) + ((tail_core, tail_place, hub_place) if first else ())
        vmem = (tail_blocks, hub_blocks, near, far, keys, duals, demand)
        vmem += (near_state, far_state, hub_state) if first else (x_all, cost_all, upper_all, ids)
        state = (key_n, width)
        if last:
            outs = [(tail_own, width), (hub_own, width), (row_n, width)]
        else:
            outs = [(tail_n, width), (hub_n, width), state, (row_n, width)]
            outs += [state, state, (row_devs * tiles, width)] if first else []
        out = call(
            functools.partial(step_kernel, first, last, sizes), smem, vmem, outs, [big, big, state], 2 * block_work
        )
        if last:
            return tuple(out)
        tail_terms, hub_terms, x_all, duals = out[:4]
        if first:
            cost_all, upper_all, ids = out[4:]


def solution(mesh):
    both = ("rows", "hub")
    in_specs = (
        P(both, None, None),
        P(both),
        P(both, None),
        P(both),
        P(both, None, None),
        P(both),
        P(both),
        P(both, None),
        P(both, None),
        P(both, None),
        P("hub", None),
        P("hub", None),
        P("hub", None),
        P(both, None),
        P(both, None),
    )
    out_specs = (P(both, None), P("hub", None), P(both, None))
    return jax.shard_map(
        on_device, mesh=mesh, in_specs=in_specs, out_specs=out_specs, check_vma=False
    )
```

```python
import functools

import jax
import jax.numpy as jnp
from jax import lax
from jax.experimental import pallas as pl
from jax.experimental.pallas import tpu as pltpu
from jax.sharding import PartitionSpec as P


ITERS = 3

primal_step = 0.25
dual_step = 0.25

VMEM = pltpu.MemorySpace.VMEM
SMEM = pltpu.MemorySpace.SMEM
HBM = pltpu.MemorySpace.HBM


def eye_mask(width):
    rows = lax.broadcasted_iota(jnp.int32, (width, width), 0)
    return rows == lax.broadcasted_iota(jnp.int32, (width, width), 1)


def adjoint_terms(blocks, block_row, wide, out):
    def step(b, _):
        product = blocks[b] * wide[block_row[b]]
        out[pl.ds(b, 1), :] = jnp.sum(product, axis=0, keepdims=True)
        return 0

    lax.fori_loop(0, blocks.shape[0], step, 0, unroll=8)


def forward_sums(blocks, block_row, extra, start, sums):
    def step(b, _):
        sums[block_row[b]] += blocks[b] * extra[pl.ds(start + b, 1), :]
        return 0

    lax.fori_loop(0, blocks.shape[0], step, 0, unroll=4)


def fill_wide(duals, wide):
    width = duals.shape[1]
    eye = eye_mask(width)
    for r in range(wide.shape[0]):
        spread = jnp.where(eye, duals[r : r + 1, :], 0.0)
        wide[r] = jnp.broadcast_to(jnp.sum(spread, axis=1, keepdims=True), (width, width))


def split_bf16(values, count):
    parts = []
    for _ in range(count):
        parts.append(values.astype(jnp.bfloat16))
        values = values - parts[-1].astype(jnp.float32)
    return parts


def gathered_image(pieces, share, ids, keys, split):
    image = None
    for slot, source in enumerate(pieces):
        picked = [source[at : at + n, :] for at, n in share]
        values = picked[0] if len(picked) == 1 else jnp.concatenate(picked, axis=0)
        count = values.shape[0]
        tiles = -(-count // keys.shape[1])
        match = [keys == ids[slot * tiles + t : slot * tiles + t + 1, :] for t in range(tiles)]
        match = match[0] if tiles == 1 else jnp.concatenate(match, axis=1)
        match = jnp.where(match[:, :count], 1.0, 0.0).astype(jnp.bfloat16)
        for part in split_bf16(values, split):
            term = jnp.dot(match, part, preferred_element_type=jnp.float32)
            image = term if image is None else image + term
    return image


def first_terms(sizes, *refs):
    _, piece, tail_own = sizes
    ins, (payload, state) = refs[:12], refs[12:14]
    wide, blocks, hub_row, hub_col, owner, slot_of, duals, x_hub, cost_hub, upper_hub, sems = refs[14:]
    width = duals.shape[1]
    hub_n, tail_n = blocks.shape[0], owner.shape[0]
    targets = [hub_row, hub_col, owner, slot_of, blocks, duals, x_hub, cost_hub, upper_hub]
    targets += [state.at[pl.ds(i * tail_own, tail_own)] for i in range(3)]
    copies = [pltpu.make_async_copy(a, b, sems.at[i]) for i, (a, b) in enumerate(zip(ins, targets))]
    first = copies.pop(5)
    first.start()
    for copy in copies:
        copy.start()
    first.wait()
    fill_wide(duals, wide)
    for copy in copies:
        copy.wait()
    adjoint_terms(blocks, hub_row, wide, payload)
    mine = lax.axis_index("rows") * piece
    for which, source in enumerate((x_hub, cost_hub, upper_hub)):
        for i in range(piece):
            at = hub_n + which * piece + i
            payload[at : at + 1, :] = source[pl.ds(mine + i, 1), :]
    lane = lax.broadcasted_iota(jnp.int32, (1, width), 1)

    def id_row(count, value):
        row = jnp.full((1, width), -1, jnp.int32)
        for b in range(count):
            row = jnp.where(lane == b, value(b), row)
        return row.astype(jnp.float32)

    at = hub_n + 3 * piece
    payload[at : at + 1, :] = id_row(hub_n, lambda b: hub_col[b])
    payload[at + 1 :, :] = jnp.zeros((payload.shape[0] - at - 1, width), jnp.float32)
    at = 3 * tail_own
    state[at : at + 1, :] = id_row(tail_n, lambda b: owner[b] * tail_own + slot_of[b])
    state[at + 1 :, :] = jnp.zeros((state.shape[0] - at - 1, width), jnp.float32)


def choose(sources, apart, at):
    value = sources[0][at, :]
    for i in range(1, len(sources)):
        value = jnp.where(apart == i, sources[i][at, :], value)
    return value


def slot_order(apart, slots):
    return (apart & 1) * (slots // 2) + (apart >> 1)


def pick_state(tail_own, owner, slot_of, *refs):
    states, (x, cost, upper, keys) = refs[:-4], refs[-4:]
    slots, width = len(states), x.shape[1]
    me = lax.axis_index("rows")

    def step(b, _):
        apart = slot_order(owner[b] ^ me, slots)
        for which, target in enumerate((x, cost, upper)):
            target[pl.ds(b, 1), :] = choose(states, apart, pl.ds(slot_of[b] + which * tail_own, 1))
        key = jnp.full((1, width), owner[b] * tail_own + slot_of[b], jnp.int32)
        keys[pl.ds(b, 1), :] = key.astype(jnp.float32)
        return 0

    lax.fori_loop(0, x.shape[0], step, 0, unroll=8)


def tail_begin(chunk, tail_row_in, blocks_in, duals, out, blocks, wide, tail_row, sems):
    row_copy = pltpu.make_async_copy(tail_row_in, tail_row, sems.at[blocks.shape[0] // chunk])
    row_copy.start()
    copies = []
    for i in range(0, blocks.shape[0], chunk):
        part = pl.ds(i, chunk)
        copies.append(pltpu.make_async_copy(blocks_in.at[part], blocks.at[part], sems.at[i // chunk]))
        copies[-1].start()
    fill_wide(duals, wide)
    row_copy.wait()
    for i, copy in enumerate(copies):
        copy.wait()

        def step(b, _):
            product = blocks[b] * wide[tail_row[b]]
            out[pl.ds(b, 1), :] = jnp.sum(product, axis=0, keepdims=True)
            return 0

        lax.fori_loop(i * chunk, (i + 1) * chunk, step, 0, unroll=4)


def tail_adjoint(tail_row, tail_blocks, wide, tail_out):
    adjoint_terms(tail_blocks, tail_row, wide, tail_out)


def gathered_ids(sizes, states, pieces, ids):
    tail_n, tail_own, hub_n, hub_devs, piece, each = sizes
    slots, width = len(pieces), ids.shape[1]
    tiles = ids.shape[0] // slots
    hub_base = float(slots * tail_own)
    lane = lax.broadcasted_iota(jnp.int32, (1, width), 1)
    for slot in range(slots):
        merged = [jnp.full((1, width), -1.0, jnp.float32)] * tiles
        rows = [(0, tail_n, states[slot][3 * tail_own : 3 * tail_own + 1, :])]
        for z in range(hub_devs):
            at = tail_n + z * each + hub_n + 3 * piece
            rows.append((tail_n + z * hub_n, hub_n, pieces[slot][at : at + 1, :] + hub_base))
        for start, count, row in rows:
            row = pltpu.roll(row, start % width, 1) if start % width else row
            for t in range(tiles):
                here = (lane >= start - t * width) & (lane < start + count - t * width)
                merged[t] = jnp.where(here, row, merged[t])
        for t in range(tiles):
            ids[slot * tiles + t : slot * tiles + t + 1, :] = merged[t]


def share_of(tail_n, hub_n, hub_devs, each):
    if each == hub_n:
        return [(0, tail_n + hub_devs * hub_n)]
    return [(0, tail_n)] + [(tail_n + z * each, hub_n) for z in range(hub_devs)]


def primal_update(image, x, cost, upper):
    x_new = jnp.minimum(jnp.maximum(x - primal_step * (cost - image), 0.0), upper)
    return x_new, 2.0 * x_new - x


def step_kernel(first, last, sizes, *refs):
    tail_n, tail_own, hub_n, hub_own, hub_devs, piece, each, slots = sizes
    refs = list(refs)
    take = lambda n: [refs.pop(0) for _ in range(n)]
    tail_row, hub_row = take(2)
    if first:
        (hub_col,) = take(1)
    tail_blocks, hub_blocks, duals, demand = take(4)
    pieces = take(slots)
    if first:
        states = take(slots)
        picked = take(4)
    else:
        x_in, cost, upper, keys, ids = take(5)
    (duals_out,) = take(1)
    if not last:
        hub_out, wide, x_out = take(3)
    if first:
        cost, upper, keys, ids = take(4)
        x_in = x_out
    sums, extra = take(2)
    width = duals.shape[1]

    if first:
        for target, source in zip((x_in, cost, upper, keys), picked):
            target[:tail_n, :] = source[...]
        me, my_hub = lax.axis_index("rows"), lax.axis_index("hub")

        def pick(b, _):
            col = hub_col[b]
            local = col % hub_own
            apart = slot_order((local // piece) ^ me, slots)
            place = tail_n + ((col // hub_own) ^ my_hub) * each + hub_n + local % piece
            at = pl.ds(tail_n + b, 1)
            for which, target in enumerate((x_in, cost, upper)):
                target[at, :] = choose(pieces, apart, pl.ds(place + which * piece, 1))
            keys[at, :] = jnp.full((1, width), slots * tail_own + col, jnp.int32).astype(jnp.float32)
            return 0

        lax.fori_loop(0, hub_n, pick, 0, unroll=8)
        gathered_ids((tail_n, tail_own, hub_n, hub_devs, piece, each), states, pieces, ids)

    image = gathered_image(pieces, share_of(tail_n, hub_n, hub_devs, each), ids, keys[...], 2)
    x_new, extrapolated = primal_update(image, x_in[...], cost[...], upper[...])
    extra[...] = extrapolated
    if not last:
        x_out[...] = x_new

    eye = eye_mask(width)
    base = duals[...] + dual_step * demand[...]
    for r in range(sums.shape[0]):
        sums[r] = jnp.where(eye, (-1.0 / dual_step) * base[r : r + 1, :], 0.0)
    forward_sums(tail_blocks, tail_row, extra, 0, sums)
    forward_sums(hub_blocks, hub_row, extra, tail_n, sums)
    for r in range(sums.shape[0]):
        total = jnp.sum(sums[r], axis=1, keepdims=True)
        value = jnp.broadcast_to(jnp.maximum(-dual_step * total, 0.0), (width, width))
        if not last:
            wide[r] = value
        duals_out[r : r + 1, :] = jnp.sum(jnp.where(eye, value, 0.0), axis=0, keepdims=True)
    if not last:
        adjoint_terms(hub_blocks, hub_row, wide, hub_out)


def own_kernel(sizes, ids, *refs):
    tail_n, hub_n, hub_devs, each, slots = sizes
    pieces, (x_tail, cost_tail, upper_tail, x_hub, cost_hub, upper_hub, tail_out, hub_out) = refs[:slots], refs[slots:]
    tail_own, width = x_tail.shape
    hub_own = x_hub.shape[0]
    tail_key = lax.broadcasted_iota(jnp.int32, (tail_own, width), 0) + lax.axis_index("rows") * tail_own
    hub_key = lax.broadcasted_iota(jnp.int32, (hub_own, width), 0) + lax.axis_index("hub") * hub_own
    keys = jnp.concatenate([tail_key, hub_key + slots * tail_own], axis=0).astype(jnp.float32)
    image = gathered_image(pieces, share_of(tail_n, hub_n, hub_devs, each), ids, keys, 2)
    tail_out[...] = primal_update(image[:tail_own], x_tail[...], cost_tail[...], upper_tail[...])[0]
    hub_out[...] = primal_update(image[tail_own:], x_hub[...], cost_hub[...], upper_hub[...])[0]


def call(kernel, smem, vmem, outs, scratch, flops, hbm=(), room=32 << 20):
    spec = lambda space, items: [pl.BlockSpec(memory_space=space)] * len(items)
    return pl.pallas_call(
        kernel,
        out_shape=[jax.ShapeDtypeStruct(s, jnp.float32) for s in outs],
        in_specs=spec(HBM, hbm) + spec(SMEM, smem) + spec(VMEM, vmem),
        out_specs=spec(VMEM, outs),
        scratch_shapes=scratch,
        compiler_params=pltpu.CompilerParams(vmem_limit_bytes=(64 << 20) - room),
        cost_estimate=pl.CostEstimate(flops=flops, bytes_accessed=0, transcendentals=0),
    )(*hbm, *smem, *vmem)


def on_device(
    tail_blocks,
    tail_row,
    tail_owner,
    tail_slot,
    hub_blocks,
    hub_row,
    hub_col,
    x_tail,
    cost_tail,
    upper_tail,
    x_hub,
    cost_hub,
    upper_hub,
    duals,
    demand,
):
    row_devs = lax.axis_size("rows")
    hub_devs = lax.axis_size("hub")
    tail_n, width = tail_blocks.shape[0], tail_blocks.shape[2]
    hub_n = hub_blocks.shape[0]
    tail_own = x_tail.shape[0]
    hub_own = x_hub.shape[0]
    row_n = duals.shape[0]
    chips = row_devs // 2
    piece = hub_own // row_devs
    assert row_devs & (row_devs - 1) == 0 and hub_devs & (hub_devs - 1) == 0
    assert piece * row_devs == hub_own and tail_n <= width

    def swap(value, axis, mask):
        count = lax.axis_size(axis)
        return lax.ppermute(value, axis, [(i, i ^ mask) for i in range(count)])

    def over_rows(value):
        near = [value] + [swap(value, "rows", 2 * m) for m in range(1, chips)]
        return near + [swap(part, "rows", 1) for part in near]

    def over_hub(value):
        return [value] + [swap(value, "hub", m) for m in reversed(range(1, hub_devs))][::-1]

    owners = tail_owner[:, 0]
    each = hub_n + -(-(3 * piece + 1) // 8) * 8
    state_n = 3 * tail_own + 8
    f32, i32 = (lambda *s: pltpu.VMEM(s, jnp.float32)), (lambda *s: pltpu.SMEM(s, jnp.int32))
    dma = lambda n: pltpu.SemaphoreType.DMA((n,))
    work = 2 * width * width
    big = (row_n, width, width)

    payload, state = call(
        functools.partial(first_terms, (row_devs, piece, tail_own)),
        (),
        (),
        [(each, width), (state_n, width)],
        [f32(*big), f32(*hub_blocks.shape), i32(hub_n), i32(hub_n), i32(tail_n), i32(tail_n), f32(row_n, width)]
        + [f32(hub_own, width)] * 3
        + [dma(12)],
        hub_n * work,
        (hub_row, hub_col, owners, tail_slot, hub_blocks, duals, x_hub, cost_hub, upper_hub)
        + (x_tail, cost_tail, upper_tail),
        8 << 20,
    )
    states = over_rows(state)
    picked = call(
        functools.partial(pick_state, tail_own),
        (owners, tail_slot),
        tuple(states),
        [(tail_n, width)] * 4,
        [],
        tail_n * width * row_devs,
    )
    own = (x_tail, cost_tail, upper_tail, x_hub, cost_hub, upper_hub)
    share = tail_n + hub_devs * hub_n
    held = (tail_n + hub_n, width)
    for iteration in range(ITERS):
        first, last = iteration == 0, iteration == ITERS - 1
        if first:
            chunk = tail_n // 6 if tail_n % 24 == 0 else tail_n
            tail_terms, tail_held = call(
                functools.partial(tail_begin, chunk),
                (),
                (duals,),
                [(tail_n, width), tail_blocks.shape],
                [f32(*big), i32(tail_n), dma(tail_n // chunk + 1)],
                tail_n * work,
                (tail_row, tail_blocks),
                16 << 20,
            )
        else:
            (tail_terms,) = call(
                tail_adjoint, (tail_row,), (tail_held, wide), [(tail_n, width)], [], tail_n * work
            )
        parts = over_hub(payload)
        pieces = over_rows(jnp.concatenate([tail_terms] + parts, axis=0))
        step_each = each if first else hub_n
        vmem = (tail_held, hub_blocks, duals, demand, *pieces)
        vmem += (*states, *picked) if first else kept
        outs = [(row_n, width)]
        if not last:
            outs += [(hub_n, width), big, held]
        if first:
            outs += [held, held, held, (row_devs * -(-share // width), width)]
        duals, *out = call(
            functools.partial(
                step_kernel,
                first,
                last,
                (tail_n, tail_own, hub_n, hub_own, hub_devs, piece, step_each, row_devs),
            ),
            (tail_row, hub_row) + ((hub_col,) if first else ()),
            vmem,
            outs,
            [f32(*big), f32(*held)],
            (tail_n + hub_n) * work,
        )
        if not last:
            payload, wide, x_all, *rest = out
            kept = (x_all, *(rest if first else kept[1:]))
        x_tail_new, x_hub_new = call(
            functools.partial(own_kernel, (tail_n, hub_n, hub_devs, step_each, row_devs)),
            (),
            (kept[-1], *pieces, *own),
            [(tail_own, width), (hub_own, width)],
            [],
            (tail_own + hub_own) * share * row_devs * width,
        )
        own = (x_tail_new, *own[1:3], x_hub_new, *own[4:])
    return own[0], own[3], duals


def solution(mesh):
    both = ("rows", "hub")
    in_specs = (
        P(both, None, None),
        P(both),
        P(both, None),
        P(both),
        P(both, None, None),
        P(both),
        P(both),
        P(both, None),
        P(both, None),
        P(both, None),
        P("hub", None),
        P("hub", None),
        P("hub", None),
        P(both, None),
        P(both, None),
    )
    out_specs = (P(both, None), P("hub", None), P(both, None))

    return jax.shard_map(on_device, mesh=mesh, in_specs=in_specs, out_specs=out_specs, check_vma=False)
```

```python
import functools

import jax
import jax.numpy as jnp
from jax import lax
from jax.experimental import pallas as pl
from jax.experimental.pallas import tpu as pltpu
from jax.sharding import PartitionSpec as P


ITERS = 3

PARTS = 4

primal_step = 0.25
dual_step = 0.25

SEED_FLOPS = 10**10

VMEM = pltpu.MemorySpace.VMEM


def eye_mask(width):
    rows = lax.broadcasted_iota(jnp.int32, (width, width), 0)
    return rows == lax.broadcasted_iota(jnp.int32, (width, width), 1)


def adjoint_terms(blocks, block_row, wide, out):
    def step(b, _):
        product = blocks[b] * wide[block_row[b]]
        out[pl.ds(b, 1), :] = jnp.sum(product, axis=0, keepdims=True)
        return 0

    lax.fori_loop(0, blocks.shape[0], step, 0, unroll=8)


def forward_sums(blocks, block_row, extra, start, sums):
    part = blocks.shape[1] // len(sums)

    def step(b, _):
        row = block_row[b]
        scale = extra[pl.ds(start + b, 1), :]
        for q, total in enumerate(sums):
            total[row] += blocks[b, q * part : (q + 1) * part, :] * scale
        return 0

    lax.fori_loop(0, blocks.shape[0], step, 0, unroll=4)


def fill_wide(duals, wide):
    width = duals.shape[1]
    eye = eye_mask(width)
    for r in range(wide.shape[0]):
        spread = jnp.where(eye, duals[r : r + 1, :], 0.0)
        wide[r] = jnp.broadcast_to(jnp.sum(spread, axis=1, keepdims=True), (width, width))


def split_bf16(values, count):
    parts = []
    for _ in range(count):
        parts.append(values.astype(jnp.bfloat16))
        values = values - parts[-1].astype(jnp.float32)
    return parts


def gathered_image(pieces, share, ids, keys, split):
    image = None
    for slot, source in enumerate(pieces):
        picked = [source[at : at + n, :] for at, n in share]
        values = picked[0] if len(picked) == 1 else jnp.concatenate(picked, axis=0)
        count = values.shape[0]
        tiles = -(-count // keys.shape[1])
        match = [keys == ids[slot * tiles + t : slot * tiles + t + 1, :] for t in range(tiles)]
        match = match[0] if tiles == 1 else jnp.concatenate(match, axis=1)
        match = jnp.where(match[:, :count], 1.0, 0.0).astype(jnp.bfloat16)
        for part in split_bf16(values, split):
            term = jnp.dot(match, part, preferred_element_type=jnp.float32)
            image = term if image is None else image + term
    return image


def to_smem(sources, targets, sems):
    copies = [pltpu.make_async_copy(a, b, sems.at[i]) for i, (a, b) in enumerate(zip(sources, targets))]
    for copy in copies:
        copy.start()
    return copies


def wait_all(copies):
    for copy in copies:
        copy.wait()


def seed(zeros):
    zeros[...] = jnp.zeros_like(zeros)


def first_terms(sizes, *refs):
    _, piece, tail_own = sizes
    indices, (zeros, blocks, duals), hub_own, tail_consts = refs[:4], refs[4:7], refs[7:10], refs[10:13]
    payload, wide, state, *scratch, sems = refs[13:]
    copies = to_smem(indices, scratch, sems)
    hub_row, hub_col, owner, slot_of = scratch
    width = duals.shape[1]
    hub_n, tail_n = blocks.shape[0], owner.shape[0]
    for which, source in enumerate(tail_consts):
        state[which * tail_own : (which + 1) * tail_own, :] = source[...]
    fill_wide(duals, wide)
    wait_all(copies)
    adjoint_terms(blocks, hub_row, wide, payload)
    mine = lax.axis_index("rows") * piece
    for which, source in enumerate(hub_own):
        for i in range(piece):
            at = hub_n + which * piece + i
            payload[at : at + 1, :] = source[pl.ds(mine + i, 1), :]
    lane = lax.broadcasted_iota(jnp.int32, (1, width), 1)

    def id_row(count, value):
        row = jnp.full((1, width), -1, jnp.int32)
        for b in range(count):
            row = jnp.where(lane == b, value(b), row)
        return row.astype(jnp.float32)

    at = hub_n + 3 * piece
    payload[at : at + 1, :] = id_row(hub_n, lambda b: hub_col[b])
    payload[at + 1 :, :] = zeros[: payload.shape[0] - at - 1, :]
    at = 3 * tail_own
    state[at : at + 1, :] = id_row(tail_n, lambda b: owner[b] * tail_own + slot_of[b])
    state[at + 1 :, :] = zeros[: state.shape[0] - at - 1, :]


def slot_order(apart, slots):
    return (apart & 1) * (slots // 2) + (apart >> 1)


def pick_rows(count, targets, keys, base, pool, where):
    def step(b, _):
        place, gap, key = where(b)
        for which, target in enumerate(targets):
            target[pl.ds(base + b, 1), :] = pool[pl.ds(place + which * gap, 1), :]
        keys[pl.ds(base + b, 1), :] = jnp.full((1, keys.shape[1]), key, jnp.int32).astype(jnp.float32)
        return 0

    lax.fori_loop(0, count, step, 0, unroll=8)


def pick_state(tail_own, *refs):
    indices, states, (x, cost, upper, keys, pool, owner, slot_of, sems) = refs[:2], refs[2:-8], refs[-8:]
    copies = to_smem(indices, (owner, slot_of), sems)
    slots, stride = len(states), 3 * tail_own
    for slot, source in enumerate(states):
        pool[slot * stride : (slot + 1) * stride, :] = source[:stride, :]
    me = lax.axis_index("rows")
    wait_all(copies)

    def where(b):
        place = slot_order(owner[b] ^ me, slots) * stride + slot_of[b]
        return place, tail_own, owner[b] * tail_own + slot_of[b]

    pick_rows(x.shape[0], (x, cost, upper), keys, 0, pool, where)


def tail_terms(own_sizes, row_in, blocks, wide, *refs):
    *own, row, sems = refs
    copies = to_smem((row_in,), (row,), sems)
    if own_sizes is None:
        (out,) = own
    else:
        out = own.pop(-3)
        own_step(own_sizes, *own)
    wait_all(copies)
    adjoint_terms(blocks, row, wide, out)


def gathered_ids(sizes, states, pieces, ids):
    tail_n, tail_own, hub_n, hub_devs, piece, each = sizes
    slots, width = len(pieces), ids.shape[1]
    tiles = ids.shape[0] // slots
    hub_base = float(slots * tail_own)
    lane = lax.broadcasted_iota(jnp.int32, (1, width), 1)
    for slot in range(slots):
        merged = [jnp.full((1, width), -1.0, jnp.float32)] * tiles
        rows = [(0, tail_n, states[slot][3 * tail_own : 3 * tail_own + 1, :])]
        for z in range(hub_devs):
            at = tail_n + z * each + hub_n + 3 * piece
            rows.append((tail_n + z * hub_n, hub_n, pieces[slot][at : at + 1, :] + hub_base))
        for start, count, row in rows:
            row = pltpu.roll(row, start % width, 1) if start % width else row
            for t in range(tiles):
                here = (lane >= start - t * width) & (lane < start + count - t * width)
                merged[t] = jnp.where(here, row, merged[t])
        for t in range(tiles):
            ids[slot * tiles + t : slot * tiles + t + 1, :] = merged[t]


def share_of(tail_n, hub_n, hub_devs, each):
    if each == hub_n:
        return [(0, tail_n + hub_devs * hub_n)]
    return [(0, tail_n)] + [(tail_n + z * each, hub_n) for z in range(hub_devs)]


def primal_update(image, x, cost, upper):
    x_new = jnp.minimum(jnp.maximum(x - primal_step * (cost - image), 0.0), upper)
    return x_new, 2.0 * x_new - x


def step_kernel(first, last, sizes, *refs):
    tail_n, tail_own, hub_n, hub_own, hub_devs, piece, each, slots = sizes
    refs = list(refs)
    take = lambda n: [refs.pop(0) for _ in range(n)]
    indices = take(3 if first else 2)
    tail_blocks, hub_blocks, duals, demand = take(4)
    pieces = take(slots)
    if first:
        states = take(slots)
        picked = take(4)
    else:
        x_in, cost, upper, keys, ids = take(5)
    if last:
        own = take(6)
    (duals_out,) = take(1)
    if last:
        own += take(2)
    else:
        hub_out, wide, x_out = take(3)
    if first:
        cost, upper, keys, ids = take(4)
        x_in = x_out
    scratch = take(len(indices))
    sems, extra = take(2)
    if first:
        (pool,) = take(1)
    sums = refs
    copies = to_smem(indices, scratch, sems)
    tail_row, hub_row = scratch[:2]
    width, part = duals.shape[1], duals.shape[1] // PARTS

    if first:
        for target, source in zip((x_in, cost, upper, keys), picked):
            target[:tail_n, :] = source[...]
        me, my_hub = lax.axis_index("rows"), lax.axis_index("hub")
        gathered_ids((tail_n, tail_own, hub_n, hub_devs, piece, each), states, pieces, ids)
        gap = each - hub_n
        for slot in range(slots):
            for z in range(hub_devs):
                to, at = (slot * hub_devs + z) * gap, tail_n + z * each + hub_n
                pool[to : to + gap, :] = pieces[slot][at : at + gap, :]
        wait_all(copies)
        hub_col = scratch[2]

        def where(b):
            col = hub_col[b]
            local = col % hub_own
            slot = slot_order((local // piece) ^ me, slots)
            place = (slot * hub_devs + ((col // hub_own) ^ my_hub)) * gap + local % piece
            return place, piece, slots * tail_own + col

        pick_rows(hub_n, (x_in, cost, upper), keys, tail_n, pool, where)

    image = gathered_image(pieces, share_of(tail_n, hub_n, hub_devs, each), ids, keys[...], 2)
    x_new, extrapolated = primal_update(image, x_in[...], cost[...], upper[...])
    extra[...] = extrapolated
    if not last:
        x_out[...] = x_new

    eye = eye_mask(width)
    base = duals[...] + dual_step * demand[...]
    for r in range(base.shape[0]):
        start = jnp.where(eye, (-1.0 / dual_step) * base[r : r + 1, :], 0.0)
        for q in range(PARTS):
            sums[q][r] = start[q * part : (q + 1) * part, :]
    if not first:
        wait_all(copies)
    forward_sums(tail_blocks, tail_row, extra, 0, sums)
    forward_sums(hub_blocks, hub_row, extra, tail_n, sums)
    for r in range(base.shape[0]):
        diagonal = jnp.zeros((1, width), jnp.float32)
        for q in range(PARTS):
            rows = slice(q * part, (q + 1) * part)
            total = jnp.sum(sums[q][r], axis=1, keepdims=True)
            value = jnp.broadcast_to(jnp.maximum(-dual_step * total, 0.0), (part, width))
            if not last:
                wide[r, rows, :] = value
            diagonal += jnp.sum(jnp.where(eye[rows, :], value, 0.0), axis=0, keepdims=True)
        duals_out[r : r + 1, :] = diagonal
    if last:
        own_step((tail_n, hub_n, hub_devs, each, slots), ids, *pieces, *own)
    else:
        adjoint_terms(hub_blocks, hub_row, wide, hub_out)


def own_step(sizes, ids, *refs):
    tail_n, hub_n, hub_devs, each, slots = sizes
    pieces, (x_tail, cost_tail, upper_tail, x_hub, cost_hub, upper_hub, tail_out, hub_out) = refs[:slots], refs[slots:]
    tail_own, width = x_tail.shape
    hub_own = x_hub.shape[0]
    tail_key = lax.broadcasted_iota(jnp.int32, (tail_own, width), 0) + lax.axis_index("rows") * tail_own
    hub_key = lax.broadcasted_iota(jnp.int32, (hub_own, width), 0) + lax.axis_index("hub") * hub_own
    keys = jnp.concatenate([tail_key, hub_key + slots * tail_own], axis=0).astype(jnp.float32)
    image = gathered_image(pieces, share_of(tail_n, hub_n, hub_devs, each), ids, keys, 2)
    tail_out[...] = primal_update(image[:tail_own], x_tail[...], cost_tail[...], upper_tail[...])[0]
    hub_out[...] = primal_update(image[tail_own:], x_hub[...], cost_hub[...], upper_hub[...])[0]


def call(kernel, ins, outs, scratch, flops):
    spec = lambda items: [pl.BlockSpec(memory_space=VMEM)] * len(items)
    return pl.pallas_call(
        kernel,
        out_shape=[jax.ShapeDtypeStruct(s, jnp.float32) for s in outs],
        in_specs=spec(ins),
        out_specs=spec(outs),
        scratch_shapes=scratch,
        compiler_params=pltpu.CompilerParams(vmem_limit_bytes=32 << 20),
        cost_estimate=pl.CostEstimate(flops=flops, bytes_accessed=0, transcendentals=0),
    )(*ins)


def on_device(
    tail_blocks,
    tail_row,
    tail_owner,
    tail_slot,
    hub_blocks,
    hub_row,
    hub_col,
    x_tail,
    cost_tail,
    upper_tail,
    x_hub,
    cost_hub,
    upper_hub,
    duals,
    demand,
):
    row_devs = lax.axis_size("rows")
    hub_devs = lax.axis_size("hub")
    tail_n, width = tail_blocks.shape[0], tail_blocks.shape[2]
    hub_n = hub_blocks.shape[0]
    tail_own = x_tail.shape[0]
    hub_own = x_hub.shape[0]
    row_n = duals.shape[0]
    chips = row_devs // 2
    piece = hub_own // row_devs
    assert row_devs & (row_devs - 1) == 0 and hub_devs & (hub_devs - 1) == 0
    assert piece * row_devs == hub_own and tail_n <= width

    def swap(value, axis, mask):
        count = lax.axis_size(axis)
        return lax.ppermute(value, axis, [(i, i ^ mask) for i in range(count)])

    def over_rows(value):
        near = [value] + [swap(value, "rows", 2 * m) for m in reversed(range(1, chips))][::-1]
        return near + [swap(part, "rows", 1) for part in near]

    def over_hub(value):
        return [value] + [swap(value, "hub", m) for m in reversed(range(1, hub_devs))][::-1]

    owners = tail_owner[:, 0]
    each = hub_n + -(-(3 * piece + 1) // 8) * 8
    state_n = 3 * tail_own + 8
    f32 = lambda *s: pltpu.VMEM(s, jnp.float32)
    ints = lambda *sizes: [pltpu.SMEM((n,), jnp.int32) for n in sizes] + [pltpu.SemaphoreType.DMA((len(sizes),))]
    work = 2 * width * width
    big = (row_n, width, width)

    (zeros,) = call(seed, (), [(8, width)], [], SEED_FLOPS)
    payload, wide, state = call(
        functools.partial(first_terms, (row_devs, piece, tail_own)),
        (hub_row, hub_col, owners, tail_slot, zeros, hub_blocks, duals)
        + (x_hub, cost_hub, upper_hub, x_tail, cost_tail, upper_tail),
        [(each, width), big, (state_n, width)],
        ints(hub_n, hub_n, tail_n, tail_n),
        hub_n * work,
    )
    states = over_rows(state)
    picked = call(
        functools.partial(pick_state, tail_own),
        (owners, tail_slot, *states),
        [(tail_n, width)] * 4,
        [f32(row_devs * 3 * tail_own, width)] + ints(tail_n, tail_n),
        tail_n * width * row_devs,
    )
    own = (x_tail, cost_tail, upper_tail, x_hub, cost_hub, upper_hub)
    own_outs = [(tail_own, width), (hub_own, width)]
    share = tail_n + hub_devs * hub_n
    held = (tail_n + hub_n, width)
    for iteration in range(ITERS):
        first, last = iteration == 0, iteration == ITERS - 1
        terms, *own_new = call(
            functools.partial(tail_terms, None if first else (tail_n, hub_n, hub_devs, step_each, row_devs)),
            (tail_row, tail_blocks, wide) + (() if first else (kept[-1], *pieces, *own)),
            [(tail_n, width)] + ([] if first else own_outs),
            ints(tail_n),
            tail_n * work,
        )
        if not first:
            own = (own_new[0], *own[1:3], own_new[1], *own[4:])
        parts = over_hub(payload)
        pieces = over_rows(jnp.concatenate([terms] + parts, axis=0))
        step_each = each if first else hub_n
        ins = (tail_row, hub_row) + (hub_col,) * first + (tail_blocks, hub_blocks, duals, demand, *pieces)
        ins += (*states, *picked) if first else kept
        ins += own if last else ()
        outs = [(row_n, width)] + (own_outs if last else [(hub_n, width), big, held])
        outs += [held, held, held, (row_devs * -(-share // width), width)] * first
        scratch = ints(tail_n, hub_n, *[hub_n] * first) + [f32(*held)]
        scratch += [f32(row_devs * hub_devs * (each - hub_n), width)] * first
        sizes = (tail_n, tail_own, hub_n, hub_own, hub_devs, piece, step_each, row_devs)
        duals, *out = call(
            functools.partial(step_kernel, first, last, sizes),
            ins,
            outs,
            scratch + [f32(row_n, width // PARTS, width)] * PARTS,
            (tail_n + hub_n) * work,
        )
        if last:
            return out[0], out[1], duals
        payload, wide, x_all, *rest = out
        kept = (x_all, *(rest if first else kept[1:]))


def solution(mesh):
    both = ("rows", "hub")
    in_specs = (
        P(both, None, None),
        P(both),
        P(both, None),
        P(both),
        P(both, None, None),
        P(both),
        P(both),
        P(both, None),
        P(both, None),
        P(both, None),
        P("hub", None),
        P("hub", None),
        P("hub", None),
        P(both, None),
        P(both, None),
    )
    out_specs = (P(both, None), P("hub", None), P(both, None))

    return jax.shard_map(on_device, mesh=mesh, in_specs=in_specs, out_specs=out_specs, check_vma=False)
```

```python
import functools

import jax
import jax.numpy as jnp
from jax import lax
from jax.experimental import pallas as pl
from jax.experimental.pallas import tpu as pltpu
from jax.sharding import PartitionSpec as P


ITERS = 3

PARTS = 4

primal_step = 0.25
dual_step = 0.25

SEED_FLOPS = 10**10

VMEM = pltpu.MemorySpace.VMEM


def eye_mask(width):
    rows = lax.broadcasted_iota(jnp.int32, (width, width), 0)
    return rows == lax.broadcasted_iota(jnp.int32, (width, width), 1)


def each_block(rows, count, group, body):
    if len(rows.shape) == 1:

        def plain(b, _):
            body(b, rows[b])
            return 0

        lax.fori_loop(0, count, plain, 0, unroll=group)
        return
    assert count % group == 0
    read = lambda first: tuple(rows[pl.ds(first + i, 1), :][0, 0] for i in range(group))

    def step(g, now):
        later = read(jnp.minimum((g + 1) * group, count - group))
        for i in range(group):
            body(g * group + i, now[i])
        return later

    lax.fori_loop(0, count // group, step, read(0))


def adjoint_terms(blocks, rows, wide, out):
    def body(b, row):
        out[pl.ds(b, 1), :] = jnp.sum(blocks[b] * wide[row], axis=0, keepdims=True)

    each_block(rows, blocks.shape[0], 8, body)


def forward_sums(blocks, rows, extra, start, sums):
    part = blocks.shape[1] // len(sums)

    def body(b, row):
        scale = extra[pl.ds(start + b, 1), :]
        for q, total in enumerate(sums):
            total[row] += blocks[b, q * part : (q + 1) * part, :] * scale

    each_block(rows, blocks.shape[0], 4, body)


def fill_wide(duals, wide):
    width = duals.shape[1]
    eye = eye_mask(width)
    for r in range(wide.shape[0]):
        spread = jnp.where(eye, duals[r : r + 1, :], 0.0)
        wide[r] = jnp.broadcast_to(jnp.sum(spread, axis=1, keepdims=True), (width, width))


def split_bf16(values, count):
    parts = []
    for _ in range(count):
        parts.append(values.astype(jnp.bfloat16))
        values = values - parts[-1].astype(jnp.float32)
    return parts


def gathered_image(pieces, share, ids, keys, split):
    image = None
    for slot, source in enumerate(pieces):
        picked = [source[at : at + n, :] for at, n in share]
        values = picked[0] if len(picked) == 1 else jnp.concatenate(picked, axis=0)
        count = values.shape[0]
        tiles = -(-count // keys.shape[1])
        match = [keys == ids[slot * tiles + t : slot * tiles + t + 1, :] for t in range(tiles)]
        match = match[0] if tiles == 1 else jnp.concatenate(match, axis=1)
        match = jnp.where(match[:, :count], 1.0, 0.0).astype(jnp.bfloat16)
        for part in split_bf16(values, split):
            term = jnp.dot(match, part, preferred_element_type=jnp.float32)
            image = term if image is None else image + term
    return image


def to_smem(sources, targets, sems):
    copies = [pltpu.make_async_copy(a, b, sems.at[i]) for i, (a, b) in enumerate(zip(sources, targets))]
    for copy in copies:
        copy.start()
    return copies


def wait_all(copies):
    for copy in copies:
        copy.wait()


def seed(zeros):
    zeros[...] = jnp.zeros_like(zeros)


def first_terms(sizes, *refs):
    _, piece, tail_own = sizes
    indices, (zeros, blocks, duals), hub_own, tail_consts = refs[:5], refs[5:8], refs[8:11], refs[11:14]
    payload, wide, state, tail_rows, hub_rows, *scratch, sems = refs[14:]
    copies = to_smem(indices, scratch, sems)
    hub_row, hub_col, owner, slot_of, tail_row = scratch
    width = duals.shape[1]
    hub_n, tail_n = blocks.shape[0], owner.shape[0]
    for which, source in enumerate(tail_consts):
        state[which * tail_own : (which + 1) * tail_own, :] = source[...]
    fill_wide(duals, wide)
    wait_all(copies)
    for source, target in ((tail_row, tail_rows), (hub_row, hub_rows)):
        for b in range(target.shape[0]):
            target[b : b + 1, :] = jnp.full((1, width), source[b], jnp.int32)
    adjoint_terms(blocks, hub_row, wide, payload)
    mine = lax.axis_index("rows") * piece
    for which, source in enumerate(hub_own):
        for i in range(piece):
            at = hub_n + which * piece + i
            payload[at : at + 1, :] = source[pl.ds(mine + i, 1), :]
    lane = lax.broadcasted_iota(jnp.int32, (1, width), 1)

    def id_row(count, value):
        row = jnp.full((1, width), -1, jnp.int32)
        for b in range(count):
            row = jnp.where(lane == b, value(b), row)
        return row.astype(jnp.float32)

    at = hub_n + 3 * piece
    payload[at : at + 1, :] = id_row(hub_n, lambda b: hub_col[b])
    payload[at + 1 :, :] = zeros[: payload.shape[0] - at - 1, :]
    at = 3 * tail_own
    state[at : at + 1, :] = id_row(tail_n, lambda b: owner[b] * tail_own + slot_of[b])
    state[at + 1 :, :] = zeros[: state.shape[0] - at - 1, :]


def slot_order(apart, slots):
    return (apart & 1) * (slots // 2) + (apart >> 1)


def pick_rows(count, targets, keys, base, pool, where):
    def step(b, _):
        place, gap, key = where(b)
        for which, target in enumerate(targets):
            target[pl.ds(base + b, 1), :] = pool[pl.ds(place + which * gap, 1), :]
        keys[pl.ds(base + b, 1), :] = jnp.full((1, keys.shape[1]), key, jnp.int32).astype(jnp.float32)
        return 0

    lax.fori_loop(0, count, step, 0, unroll=8)


def pick_state(tail_own, *refs):
    indices, states, (x, cost, upper, keys, pool, owner, slot_of, sems) = refs[:2], refs[2:-8], refs[-8:]
    copies = to_smem(indices, (owner, slot_of), sems)
    slots, stride = len(states), 3 * tail_own
    for slot, source in enumerate(states):
        pool[slot * stride : (slot + 1) * stride, :] = source[:stride, :]
    me = lax.axis_index("rows")
    wait_all(copies)

    def where(b):
        place = slot_order(owner[b] ^ me, slots) * stride + slot_of[b]
        return place, tail_own, owner[b] * tail_own + slot_of[b]

    pick_rows(x.shape[0], (x, cost, upper), keys, 0, pool, where)


def tail_terms(own_sizes, rows, blocks, wide, *refs):
    own = list(refs)
    out = own.pop(-1 if own_sizes is None else -3)
    adjoint_terms(blocks, rows, wide, out)
    if own_sizes is not None:
        own_step(own_sizes, *own)


def gathered_ids(sizes, states, pieces, ids):
    tail_n, tail_own, hub_n, hub_devs, piece, each = sizes
    slots, width = len(pieces), ids.shape[1]
    tiles = ids.shape[0] // slots
    hub_base = float(slots * tail_own)
    lane = lax.broadcasted_iota(jnp.int32, (1, width), 1)
    for slot in range(slots):
        merged = [jnp.full((1, width), -1.0, jnp.float32)] * tiles
        rows = [(0, tail_n, states[slot][3 * tail_own : 3 * tail_own + 1, :])]
        for z in range(hub_devs):
            at = tail_n + z * each + hub_n + 3 * piece
            rows.append((tail_n + z * hub_n, hub_n, pieces[slot][at : at + 1, :] + hub_base))
        for start, count, row in rows:
            row = pltpu.roll(row, start % width, 1) if start % width else row
            for t in range(tiles):
                here = (lane >= start - t * width) & (lane < start + count - t * width)
                merged[t] = jnp.where(here, row, merged[t])
        for t in range(tiles):
            ids[slot * tiles + t : slot * tiles + t + 1, :] = merged[t]


def share_of(tail_n, hub_n, hub_devs, each):
    if each == hub_n:
        return [(0, tail_n + hub_devs * hub_n)]
    return [(0, tail_n)] + [(tail_n + z * each, hub_n) for z in range(hub_devs)]


def primal_update(image, x, cost, upper):
    x_new = jnp.minimum(jnp.maximum(x - primal_step * (cost - image), 0.0), upper)
    return x_new, 2.0 * x_new - x


def step_kernel(first, last, sizes, *refs):
    tail_n, tail_own, hub_n, hub_own, hub_devs, piece, each, slots = sizes
    refs = list(refs)
    take = lambda n: [refs.pop(0) for _ in range(n)]
    indices = take(3 if first else 2)
    hub_rows, tail_blocks, hub_blocks, duals, demand = take(5)
    pieces = take(slots)
    if first:
        states = take(slots)
        picked = take(4)
    else:
        x_in, cost, upper, keys, ids = take(5)
    if last:
        own = take(6)
    (duals_out,) = take(1)
    if last:
        own += take(2)
    else:
        hub_out, wide, x_out = take(3)
    if first:
        cost, upper, keys, ids = take(4)
        x_in = x_out
    scratch = take(len(indices))
    sems, extra = take(2)
    if first:
        (pool,) = take(1)
    sums = refs
    copies = to_smem(indices, scratch, sems)
    tail_row, hub_row = scratch[:2]
    width, part = duals.shape[1], duals.shape[1] // PARTS

    if first:
        for target, source in zip((x_in, cost, upper, keys), picked):
            target[:tail_n, :] = source[...]
        me, my_hub = lax.axis_index("rows"), lax.axis_index("hub")
        gathered_ids((tail_n, tail_own, hub_n, hub_devs, piece, each), states, pieces, ids)
        gap = each - hub_n
        for slot in range(slots):
            for z in range(hub_devs):
                to, at = (slot * hub_devs + z) * gap, tail_n + z * each + hub_n
                pool[to : to + gap, :] = pieces[slot][at : at + gap, :]
        wait_all(copies)
        hub_col = scratch[2]

        def where(b):
            col = hub_col[b]
            local = col % hub_own
            slot = slot_order((local // piece) ^ me, slots)
            place = (slot * hub_devs + ((col // hub_own) ^ my_hub)) * gap + local % piece
            return place, piece, slots * tail_own + col

        pick_rows(hub_n, (x_in, cost, upper), keys, tail_n, pool, where)

    image = gathered_image(pieces, share_of(tail_n, hub_n, hub_devs, each), ids, keys[...], 2)
    x_new, extrapolated = primal_update(image, x_in[...], cost[...], upper[...])
    extra[...] = extrapolated
    if not last:
        x_out[...] = x_new

    eye = eye_mask(width)
    base = duals[...] + dual_step * demand[...]
    for r in range(base.shape[0]):
        start = jnp.where(eye, (-1.0 / dual_step) * base[r : r + 1, :], 0.0)
        for q in range(PARTS):
            sums[q][r] = start[q * part : (q + 1) * part, :]
    forward_sums(hub_blocks, hub_row if first else hub_rows, extra, tail_n, sums)
    if not first:
        wait_all(copies)
    forward_sums(tail_blocks, tail_row, extra, 0, sums)
    for r in range(base.shape[0]):
        diagonal = jnp.zeros((1, width), jnp.float32)
        for q in range(PARTS):
            rows = slice(q * part, (q + 1) * part)
            total = jnp.sum(sums[q][r], axis=1, keepdims=True)
            value = jnp.broadcast_to(jnp.maximum(-dual_step * total, 0.0), (part, width))
            if not last:
                wide[r, rows, :] = value
            diagonal += jnp.sum(jnp.where(eye[rows, :], value, 0.0), axis=0, keepdims=True)
        duals_out[r : r + 1, :] = diagonal
    if last:
        own_step((tail_n, hub_n, hub_devs, each, slots), ids, *pieces, *own)
    else:
        adjoint_terms(hub_blocks, hub_row, wide, hub_out)


def own_step(sizes, ids, *refs):
    tail_n, hub_n, hub_devs, each, slots = sizes
    pieces, (x_tail, cost_tail, upper_tail, x_hub, cost_hub, upper_hub, tail_out, hub_out) = refs[:slots], refs[slots:]
    tail_own, width = x_tail.shape
    hub_own = x_hub.shape[0]
    tail_key = lax.broadcasted_iota(jnp.int32, (tail_own, width), 0) + lax.axis_index("rows") * tail_own
    hub_key = lax.broadcasted_iota(jnp.int32, (hub_own, width), 0) + lax.axis_index("hub") * hub_own
    keys = jnp.concatenate([tail_key, hub_key + slots * tail_own], axis=0).astype(jnp.float32)
    image = gathered_image(pieces, share_of(tail_n, hub_n, hub_devs, each), ids, keys, 2)
    tail_out[...] = primal_update(image[:tail_own], x_tail[...], cost_tail[...], upper_tail[...])[0]
    hub_out[...] = primal_update(image[tail_own:], x_hub[...], cost_hub[...], upper_hub[...])[0]


def call(kernel, ins, outs, scratch, flops):
    def shape(*sizes):
        if isinstance(sizes[-1], int):
            return jax.ShapeDtypeStruct(sizes, jnp.float32)
        return jax.ShapeDtypeStruct(sizes[:-1], sizes[-1])

    spec = lambda items: [pl.BlockSpec(memory_space=VMEM)] * len(items)
    return pl.pallas_call(
        kernel,
        out_shape=[shape(*s) for s in outs],
        in_specs=spec(ins),
        out_specs=spec(outs),
        scratch_shapes=scratch,
        compiler_params=pltpu.CompilerParams(vmem_limit_bytes=32 << 20),
        cost_estimate=pl.CostEstimate(flops=flops, bytes_accessed=0, transcendentals=0),
    )(*ins)


def on_device(
    tail_blocks,
    tail_row,
    tail_owner,
    tail_slot,
    hub_blocks,
    hub_row,
    hub_col,
    x_tail,
    cost_tail,
    upper_tail,
    x_hub,
    cost_hub,
    upper_hub,
    duals,
    demand,
):
    row_devs = lax.axis_size("rows")
    hub_devs = lax.axis_size("hub")
    tail_n, width = tail_blocks.shape[0], tail_blocks.shape[2]
    hub_n = hub_blocks.shape[0]
    tail_own = x_tail.shape[0]
    hub_own = x_hub.shape[0]
    row_n = duals.shape[0]
    chips = row_devs // 2
    piece = hub_own // row_devs
    assert row_devs & (row_devs - 1) == 0 and hub_devs & (hub_devs - 1) == 0
    assert piece * row_devs == hub_own and tail_n <= width

    def swap(value, axis, mask):
        count = lax.axis_size(axis)
        return lax.ppermute(value, axis, [(i, i ^ mask) for i in range(count)])

    def over_rows(value):
        near = [value] + [swap(value, "rows", 2 * m) for m in reversed(range(1, chips))][::-1]
        return near + [swap(part, "rows", 1) for part in near]

    def over_hub(value):
        return [value] + [swap(value, "hub", m) for m in reversed(range(1, hub_devs))][::-1]

    owners = tail_owner[:, 0]
    each = hub_n + -(-(3 * piece + 1) // 8) * 8
    state_n = 3 * tail_own + 8
    f32 = lambda *s: pltpu.VMEM(s, jnp.float32)
    ints = lambda *sizes: [pltpu.SMEM((n,), jnp.int32) for n in sizes] + [pltpu.SemaphoreType.DMA((len(sizes),))]
    work = 2 * width * width
    big = (row_n, width, width)

    (zeros,) = call(seed, (), [(8, width)], [], SEED_FLOPS)
    payload, wide, state, tail_rows, hub_rows = call(
        functools.partial(first_terms, (row_devs, piece, tail_own)),
        (hub_row, hub_col, owners, tail_slot, tail_row, zeros, hub_blocks, duals)
        + (x_hub, cost_hub, upper_hub, x_tail, cost_tail, upper_tail),
        [(each, width), big, (state_n, width), (tail_n, width, jnp.int32), (hub_n, width, jnp.int32)],
        ints(hub_n, hub_n, tail_n, tail_n, tail_n),
        hub_n * work,
    )
    states = over_rows(state)
    picked = call(
        functools.partial(pick_state, tail_own),
        (owners, tail_slot, *states),
        [(tail_n, width)] * 4,
        [f32(row_devs * 3 * tail_own, width)] + ints(tail_n, tail_n),
        tail_n * width * row_devs,
    )
    own = (x_tail, cost_tail, upper_tail, x_hub, cost_hub, upper_hub)
    own_outs = [(tail_own, width), (hub_own, width)]
    share = tail_n + hub_devs * hub_n
    held = (tail_n + hub_n, width)
    for iteration in range(ITERS):
        first, last = iteration == 0, iteration == ITERS - 1
        terms, *own_new = call(
            functools.partial(tail_terms, None if first else (tail_n, hub_n, hub_devs, step_each, row_devs)),
            (tail_rows, tail_blocks, wide) + (() if first else (kept[-1], *pieces, *own)),
            [(tail_n, width)] + ([] if first else own_outs),
            [],
            tail_n * work,
        )
        if not first:
            own = (own_new[0], *own[1:3], own_new[1], *own[4:])
        parts = over_hub(payload)
        pieces = over_rows(jnp.concatenate([terms] + parts, axis=0))
        step_each = each if first else hub_n
        ins = (tail_row, hub_row) + (hub_col,) * first + (hub_rows, tail_blocks, hub_blocks, duals, demand, *pieces)
        ins += (*states, *picked) if first else kept
        ins += own if last else ()
        outs = [(row_n, width)] + (own_outs if last else [(hub_n, width), big, held])
        outs += [held, held, held, (row_devs * -(-share // width), width)] * first
        scratch = ints(tail_n, hub_n, *[hub_n] * first) + [f32(*held)]
        scratch += [f32(row_devs * hub_devs * (each - hub_n), width)] * first
        sizes = (tail_n, tail_own, hub_n, hub_own, hub_devs, piece, step_each, row_devs)
        duals, *out = call(
            functools.partial(step_kernel, first, last, sizes),
            ins,
            outs,
            scratch + [f32(row_n, width // PARTS, width)] * PARTS,
            (tail_n + hub_n) * work,
        )
        if last:
            return out[0], out[1], duals
        payload, wide, x_all, *rest = out
        kept = (x_all, *(rest if first else kept[1:]))


def solution(mesh):
    both = ("rows", "hub")
    in_specs = (
        P(both, None, None),
        P(both),
        P(both, None),
        P(both),
        P(both, None, None),
        P(both),
        P(both),
        P(both, None),
        P(both, None),
        P(both, None),
        P("hub", None),
        P("hub", None),
        P("hub", None),
        P(both, None),
        P(both, None),
    )
    out_specs = (P(both, None), P("hub", None), P(both, None))

    return jax.shard_map(on_device, mesh=mesh, in_specs=in_specs, out_specs=out_specs, check_vma=False)
```

```python
import functools

import jax
import jax.numpy as jnp
from jax import lax
from jax.experimental import pallas as pl
from jax.experimental.pallas import tpu as pltpu
from jax.sharding import PartitionSpec as P


ITERS = 3

PARTS = 4

primal_step = 0.25
dual_step = 0.25

SEED_FLOPS = 10**10

VMEM = pltpu.MemorySpace.VMEM


def eye_mask(width):
    rows = lax.broadcasted_iota(jnp.int32, (width, width), 0)
    return rows == lax.broadcasted_iota(jnp.int32, (width, width), 1)


def each_block(rows, count, group, body):
    if len(rows.shape) == 1:

        def plain(b, _):
            body(b, rows[b])
            return 0

        lax.fori_loop(0, count, plain, 0, unroll=group)
        return
    assert count % group == 0
    read = lambda first: tuple(rows[pl.ds(first + i, 1), :][0, 0] for i in range(group))

    def step(g, now):
        later = read(jnp.minimum((g + 1) * group, count - group))
        for i in range(group):
            body(g * group + i, now[i])
        return later

    lax.fori_loop(0, count // group, step, read(0))


def adjoint_terms(blocks, rows, wide, out):
    def body(b, row):
        out[pl.ds(b, 1), :] = jnp.sum(blocks[b] * wide[row], axis=0, keepdims=True)

    each_block(rows, blocks.shape[0], 8, body)


def forward_sums(blocks, rows, extra, start, sums):
    part = blocks.shape[1] // len(sums)

    def body(b, row):
        scale = extra[pl.ds(start + b, 1), :]
        for q, total in enumerate(sums):
            total[row] += blocks[b, q * part : (q + 1) * part, :] * scale

    each_block(rows, blocks.shape[0], 4, body)


def fill_wide(duals, wide):
    width = duals.shape[1]
    eye = eye_mask(width)
    for r in range(wide.shape[0]):
        spread = jnp.where(eye, duals[r : r + 1, :], 0.0)
        wide[r] = jnp.broadcast_to(jnp.sum(spread, axis=1, keepdims=True), (width, width))


def split_bf16(values, count):
    parts = []
    for _ in range(count):
        parts.append(values.astype(jnp.bfloat16))
        values = values - parts[-1].astype(jnp.float32)
    return parts


def gathered_image(pieces, share, ids, keys, split):
    image = None
    for slot, source in enumerate(pieces):
        picked = [source[at : at + n, :] for at, n in share]
        values = picked[0] if len(picked) == 1 else jnp.concatenate(picked, axis=0)
        count = values.shape[0]
        tiles = -(-count // keys.shape[1])
        match = [keys == ids[slot * tiles + t : slot * tiles + t + 1, :] for t in range(tiles)]
        match = match[0] if tiles == 1 else jnp.concatenate(match, axis=1)
        match = jnp.where(match[:, :count], 1.0, 0.0).astype(jnp.bfloat16)
        term = jnp.dot(match, jnp.concatenate(split_bf16(values, split), axis=1), preferred_element_type=jnp.float32)
        image = term if image is None else image + term
    width = keys.shape[1]
    image = sum(image[:, i * width : (i + 1) * width] for i in range(split))
    return image


def to_smem(sources, targets, sems):
    copies = [pltpu.make_async_copy(a, b, sems.at[i]) for i, (a, b) in enumerate(zip(sources, targets))]
    for copy in copies:
        copy.start()
    return copies


def wait_all(copies):
    for copy in copies:
        copy.wait()


def seed(zeros):
    zeros[...] = jnp.zeros_like(zeros)


def first_terms(sizes, *refs):
    _, piece, tail_own = sizes
    indices, (zeros, blocks, duals), hub_own, tail_consts = refs[:5], refs[5:8], refs[8:11], refs[11:14]
    payload, wide, state, tail_rows, hub_rows, *scratch, sems = refs[14:]
    copies = to_smem(indices, scratch, sems)
    hub_row, hub_col, owner, slot_of, tail_row = scratch
    width = duals.shape[1]
    hub_n, tail_n = blocks.shape[0], owner.shape[0]
    for which, source in enumerate(tail_consts):
        state[which * tail_own : (which + 1) * tail_own, :] = source[...]
    fill_wide(duals, wide)
    wait_all(copies)
    for source, target in ((tail_row, tail_rows), (hub_row, hub_rows)):
        for b in range(target.shape[0]):
            target[b : b + 1, :] = jnp.full((1, width), source[b], jnp.int32)
    adjoint_terms(blocks, hub_row, wide, payload)
    mine = lax.axis_index("rows") * piece
    for which, source in enumerate(hub_own):
        for i in range(piece):
            at = hub_n + which * piece + i
            payload[at : at + 1, :] = source[pl.ds(mine + i, 1), :]
    lane = lax.broadcasted_iota(jnp.int32, (1, width), 1)

    def id_row(count, value):
        row = jnp.full((1, width), -1, jnp.int32)
        for b in range(count):
            row = jnp.where(lane == b, value(b), row)
        return row.astype(jnp.float32)

    at = hub_n + 3 * piece
    payload[at : at + 1, :] = id_row(hub_n, lambda b: hub_col[b])
    payload[at + 1 :, :] = zeros[: payload.shape[0] - at - 1, :]
    at = 3 * tail_own
    state[at : at + 1, :] = id_row(tail_n, lambda b: owner[b] * tail_own + slot_of[b])
    state[at + 1 :, :] = zeros[: state.shape[0] - at - 1, :]


def slot_order(apart, slots):
    return (apart & 1) * (slots // 2) + (apart >> 1)


def pick_rows(count, targets, keys, base, pool, where):
    def step(b, _):
        place, gap, key = where(b)
        for which, target in enumerate(targets):
            target[pl.ds(base + b, 1), :] = pool[pl.ds(place + which * gap, 1), :]
        keys[pl.ds(base + b, 1), :] = jnp.full((1, keys.shape[1]), key, jnp.int32).astype(jnp.float32)
        return 0

    lax.fori_loop(0, count, step, 0, unroll=8)


def pick_state(tail_own, *refs):
    indices, states, (x, cost, upper, keys, pool, owner, slot_of, sems) = refs[:2], refs[2:-8], refs[-8:]
    copies = to_smem(indices, (owner, slot_of), sems)
    slots, stride = len(states), 3 * tail_own
    for slot, source in enumerate(states):
        pool[slot * stride : (slot + 1) * stride, :] = source[:stride, :]
    me = lax.axis_index("rows")
    wait_all(copies)

    def where(b):
        place = slot_order(owner[b] ^ me, slots) * stride + slot_of[b]
        return place, tail_own, owner[b] * tail_own + slot_of[b]

    pick_rows(x.shape[0], (x, cost, upper), keys, 0, pool, where)


def tail_terms(own_sizes, rows, blocks, wide, *refs):
    own = list(refs)
    out = own.pop(-1 if own_sizes is None else -3)
    adjoint_terms(blocks, rows, wide, out)
    if own_sizes is not None:
        own_step(own_sizes, *own)


def gathered_ids(sizes, states, pieces, ids):
    tail_n, tail_own, hub_n, hub_devs, piece, each = sizes
    slots, width = len(pieces), ids.shape[1]
    tiles = ids.shape[0] // slots
    hub_base = float(slots * tail_own)
    lane = lax.broadcasted_iota(jnp.int32, (1, width), 1)
    for slot in range(slots):
        merged = [jnp.full((1, width), -1.0, jnp.float32)] * tiles
        rows = [(0, tail_n, states[slot][3 * tail_own : 3 * tail_own + 1, :])]
        for z in range(hub_devs):
            at = tail_n + z * each + hub_n + 3 * piece
            rows.append((tail_n + z * hub_n, hub_n, pieces[slot][at : at + 1, :] + hub_base))
        for start, count, row in rows:
            row = pltpu.roll(row, start % width, 1) if start % width else row
            for t in range(tiles):
                here = (lane >= start - t * width) & (lane < start + count - t * width)
                merged[t] = jnp.where(here, row, merged[t])
        for t in range(tiles):
            ids[slot * tiles + t : slot * tiles + t + 1, :] = merged[t]


def share_of(tail_n, hub_n, hub_devs, each):
    if each == hub_n:
        return [(0, tail_n + hub_devs * hub_n)]
    return [(0, tail_n)] + [(tail_n + z * each, hub_n) for z in range(hub_devs)]


def primal_update(image, x, cost, upper):
    x_new = jnp.minimum(jnp.maximum(x - primal_step * (cost - image), 0.0), upper)
    return x_new, 2.0 * x_new - x


def step_kernel(first, last, sizes, *refs):
    tail_n, tail_own, hub_n, hub_own, hub_devs, piece, each, slots = sizes
    refs = list(refs)
    take = lambda n: [refs.pop(0) for _ in range(n)]
    indices = take(3 if first else 2)
    hub_rows, tail_blocks, hub_blocks, duals, demand = take(5)
    pieces = take(slots)
    if first:
        states = take(slots)
        picked = take(4)
    else:
        x_in, cost, upper, keys, ids = take(5)
    if last:
        own = take(6)
    (duals_out,) = take(1)
    if last:
        own += take(2)
    else:
        hub_out, wide, x_out = take(3)
    if first:
        cost, upper, keys, ids = take(4)
        x_in = x_out
    scratch = take(len(indices))
    sems, extra = take(2)
    if first:
        (pool,) = take(1)
    sums = refs
    copies = to_smem(indices, scratch, sems)
    tail_row, hub_row = scratch[:2]
    width, part = duals.shape[1], duals.shape[1] // PARTS

    if first:
        for target, source in zip((x_in, cost, upper, keys), picked):
            target[:tail_n, :] = source[...]
        me, my_hub = lax.axis_index("rows"), lax.axis_index("hub")
        gathered_ids((tail_n, tail_own, hub_n, hub_devs, piece, each), states, pieces, ids)
        gap = each - hub_n
        for slot in range(slots):
            for z in range(hub_devs):
                to, at = (slot * hub_devs + z) * gap, tail_n + z * each + hub_n
                pool[to : to + gap, :] = pieces[slot][at : at + gap, :]
        wait_all(copies)
        hub_col = scratch[2]

        def where(b):
            col = hub_col[b]
            local = col % hub_own
            slot = slot_order((local // piece) ^ me, slots)
            place = (slot * hub_devs + ((col // hub_own) ^ my_hub)) * gap + local % piece
            return place, piece, slots * tail_own + col

        pick_rows(hub_n, (x_in, cost, upper), keys, tail_n, pool, where)

    image = gathered_image(pieces, share_of(tail_n, hub_n, hub_devs, each), ids, keys[...], 2)
    x_new, extrapolated = primal_update(image, x_in[...], cost[...], upper[...])
    extra[...] = extrapolated
    if not last:
        x_out[...] = x_new

    eye = eye_mask(width)
    base = duals[...] + dual_step * demand[...]
    for r in range(base.shape[0]):
        start = jnp.where(eye, (-1.0 / dual_step) * base[r : r + 1, :], 0.0)
        for q in range(PARTS):
            sums[q][r] = start[q * part : (q + 1) * part, :]
    forward_sums(hub_blocks, hub_row if first else hub_rows, extra, tail_n, sums)
    if not first:
        wait_all(copies)
    forward_sums(tail_blocks, tail_row, extra, 0, sums)
    for r in range(base.shape[0]):
        diagonal = jnp.zeros((1, width), jnp.float32)
        for q in range(PARTS):
            rows = slice(q * part, (q + 1) * part)
            total = jnp.sum(sums[q][r], axis=1, keepdims=True)
            value = jnp.broadcast_to(jnp.maximum(-dual_step * total, 0.0), (part, width))
            if not last:
                wide[r, rows, :] = value
            diagonal += jnp.sum(jnp.where(eye[rows, :], value, 0.0), axis=0, keepdims=True)
        duals_out[r : r + 1, :] = diagonal
    if last:
        own_step((tail_n, hub_n, hub_devs, each, slots), ids, *pieces, *own)
    else:
        adjoint_terms(hub_blocks, hub_row, wide, hub_out)


def own_step(sizes, ids, *refs):
    tail_n, hub_n, hub_devs, each, slots = sizes
    pieces, (x_tail, cost_tail, upper_tail, x_hub, cost_hub, upper_hub, tail_out, hub_out) = refs[:slots], refs[slots:]
    tail_own, width = x_tail.shape
    hub_own = x_hub.shape[0]
    tail_key = lax.broadcasted_iota(jnp.int32, (tail_own, width), 0) + lax.axis_index("rows") * tail_own
    hub_key = lax.broadcasted_iota(jnp.int32, (hub_own, width), 0) + lax.axis_index("hub") * hub_own
    keys = jnp.concatenate([tail_key, hub_key + slots * tail_own], axis=0).astype(jnp.float32)
    image = gathered_image(pieces, share_of(tail_n, hub_n, hub_devs, each), ids, keys, 2)
    tail_out[...] = primal_update(image[:tail_own], x_tail[...], cost_tail[...], upper_tail[...])[0]
    hub_out[...] = primal_update(image[tail_own:], x_hub[...], cost_hub[...], upper_hub[...])[0]


def call(kernel, ins, outs, scratch, flops):
    def shape(*sizes):
        if isinstance(sizes[-1], int):
            return jax.ShapeDtypeStruct(sizes, jnp.float32)
        return jax.ShapeDtypeStruct(sizes[:-1], sizes[-1])

    spec = lambda items: [pl.BlockSpec(memory_space=VMEM)] * len(items)
    return pl.pallas_call(
        kernel,
        out_shape=[shape(*s) for s in outs],
        in_specs=spec(ins),
        out_specs=spec(outs),
        scratch_shapes=scratch,
        compiler_params=pltpu.CompilerParams(vmem_limit_bytes=32 << 20),
        cost_estimate=pl.CostEstimate(flops=flops, bytes_accessed=0, transcendentals=0),
    )(*ins)


def on_device(
    tail_blocks,
    tail_row,
    tail_owner,
    tail_slot,
    hub_blocks,
    hub_row,
    hub_col,
    x_tail,
    cost_tail,
    upper_tail,
    x_hub,
    cost_hub,
    upper_hub,
    duals,
    demand,
):
    row_devs = lax.axis_size("rows")
    hub_devs = lax.axis_size("hub")
    tail_n, width = tail_blocks.shape[0], tail_blocks.shape[2]
    hub_n = hub_blocks.shape[0]
    tail_own = x_tail.shape[0]
    hub_own = x_hub.shape[0]
    row_n = duals.shape[0]
    chips = row_devs // 2
    piece = hub_own // row_devs
    assert row_devs & (row_devs - 1) == 0 and hub_devs & (hub_devs - 1) == 0
    assert piece * row_devs == hub_own and tail_n <= width

    def swap(value, axis, mask):
        count = lax.axis_size(axis)
        return lax.ppermute(value, axis, [(i, i ^ mask) for i in range(count)])

    def over_rows(value):
        near = [value] + [swap(value, "rows", 2 * m) for m in reversed(range(1, chips))][::-1]
        return near + [swap(part, "rows", 1) for part in near]

    def over_hub(value):
        return [value] + [swap(value, "hub", m) for m in reversed(range(1, hub_devs))][::-1]

    owners = tail_owner[:, 0]
    each = hub_n + -(-(3 * piece + 1) // 8) * 8
    state_n = 3 * tail_own + 8
    f32 = lambda *s: pltpu.VMEM(s, jnp.float32)
    ints = lambda *sizes: [pltpu.SMEM((n,), jnp.int32) for n in sizes] + [pltpu.SemaphoreType.DMA((len(sizes),))]
    work = 2 * width * width
    big = (row_n, width, width)

    (zeros,) = call(seed, (), [(8, width)], [], SEED_FLOPS)
    payload, wide, state, tail_rows, hub_rows = call(
        functools.partial(first_terms, (row_devs, piece, tail_own)),
        (hub_row, hub_col, owners, tail_slot, tail_row, zeros, hub_blocks, duals)
        + (x_hub, cost_hub, upper_hub, x_tail, cost_tail, upper_tail),
        [(each, width), big, (state_n, width), (tail_n, width, jnp.int32), (hub_n, width, jnp.int32)],
        ints(hub_n, hub_n, tail_n, tail_n, tail_n),
        hub_n * work,
    )
    states = over_rows(state)
    picked = call(
        functools.partial(pick_state, tail_own),
        (owners, tail_slot, *states),
        [(tail_n, width)] * 4,
        [f32(row_devs * 3 * tail_own, width)] + ints(tail_n, tail_n),
        tail_n * width * row_devs,
    )
    own = (x_tail, cost_tail, upper_tail, x_hub, cost_hub, upper_hub)
    own_outs = [(tail_own, width), (hub_own, width)]
    share = tail_n + hub_devs * hub_n
    held = (tail_n + hub_n, width)
    for iteration in range(ITERS):
        first, last = iteration == 0, iteration == ITERS - 1
        terms, *own_new = call(
            functools.partial(tail_terms, None if first else (tail_n, hub_n, hub_devs, step_each, row_devs)),
            (tail_rows, tail_blocks, wide) + (() if first else (kept[-1], *pieces, *own)),
            [(tail_n, width)] + ([] if first else own_outs),
            [],
            tail_n * work,
        )
        if not first:
            own = (own_new[0], *own[1:3], own_new[1], *own[4:])
        parts = over_hub(payload)
        pieces = over_rows(jnp.concatenate([terms] + parts, axis=0))
        step_each = each if first else hub_n
        ins = (tail_row, hub_row) + (hub_col,) * first + (hub_rows, tail_blocks, hub_blocks, duals, demand, *pieces)
        ins += (*states, *picked) if first else kept
        ins += own if last else ()
        outs = [(row_n, width)] + (own_outs if last else [(hub_n, width), big, held])
        outs += [held, held, held, (row_devs * -(-share // width), width)] * first
        scratch = ints(tail_n, hub_n, *[hub_n] * first) + [f32(*held)]
        scratch += [f32(row_devs * hub_devs * (each - hub_n), width)] * first
        sizes = (tail_n, tail_own, hub_n, hub_own, hub_devs, piece, step_each, row_devs)
        duals, *out = call(
            functools.partial(step_kernel, first, last, sizes),
            ins,
            outs,
            scratch + [f32(row_n, width // PARTS, width)] * PARTS,
            (tail_n + hub_n) * work,
        )
        if last:
            return out[0], out[1], duals
        payload, wide, x_all, *rest = out
        kept = (x_all, *(rest if first else kept[1:]))


def solution(mesh):
    both = ("rows", "hub")
    in_specs = (
        P(both, None, None),
        P(both),
        P(both, None),
        P(both),
        P(both, None, None),
        P(both),
        P(both),
        P(both, None),
        P(both, None),
        P(both, None),
        P("hub", None),
        P("hub", None),
        P("hub", None),
        P(both, None),
        P(both, None),
    )
    out_specs = (P(both, None), P("hub", None), P(both, None))

    return jax.shard_map(on_device, mesh=mesh, in_specs=in_specs, out_specs=out_specs, check_vma=False)
```
